768 devices in a mesh: grp: 96 (over z, y), lane: 8 (over x, core).
Axes of the slice: x: 4, y: 8, z: 12, core: 2. Of those that a mesh axis runs over, the one named last changes fastest.
Arguments:
- grad_pooled: bfloat16 [98304, 32, 256], P(('grp', 'lane')), may hold values from -16 to 16
- bag_len: int32 [98304, 32], P(('grp', 'lane')), may hold values from 1 to 8
- lookup_slot: int32 [98304, 32, 8], P('grp', 'lane'), may hold values from -1 to 191, as said below
- slot_row: int32 [96, 8, 96, 2], P('grp', 'lane'), may hold values from 0 to 1023, as said below
- weights: float32 [32, 24576, 256], P('lane', 'grp'), may hold values from -6 to 6
- accum: float32 [32, 24576], P('lane', 'grp'), may hold values from 0.05 to 0.5
Outputs:
- new_weights: float32 [32, 24576, 256], P('lane', 'grp')
- new_accum: float32 [32, 24576], P('lane', 'grp')
The draws below stay inside these ranges and needn't reach their ends.
Inputs may be any that keep to these rules, and one draw needn't show every extreme that they name: `lookup_slot`: position j of bag (b, t) holds -1 when j >= bag_len[b, t] and otherwise a slot number s; the row slot_row[s // 2, t // 4, g, s % 2], with g the group of sample b, lies in local table t % 4. `slot_row`: several slots, also from different groups, may name the same row.
All inputs are finite; a program needn't handle non-finite values.
Results may differ from the reference program's by a relative error of at most 0.0035.
Values may be sent and summed in bfloat16 or wider, within the bound.
No kernel may reach another device: no remote copies, remote signals or barrier semaphores. Data moves between devices by JAX's collectives and lax.ppermute only.
A program may use at most 32 MiB of HBM per device.

```python
import math
import jax
import jax.numpy as jnp
from jax import lax

EMBED = 256
TABLES_DEV = 4
BAG_MAX = 8
SLOTS_PEER = 2
BATCH_DEV = 128
ROWS_DEV = 256
TABLES = 32
BATCH = 98304
ROWS = 24576
SLOTS = 192
N_GRP = 96
N_LANE = 8
DEVICES = 768


def layout_keys(key):
    return jax.random.split(jax.random.fold_in(key, 913), 9)


def draw_grad_pooled(key, part):
    level_keys = jax.random.split(jax.random.fold_in(key, 421), 3)
    shape = (BATCH, TABLES, EMBED)
    level = jax.random.uniform(level_keys[0], (1, TABLES, 1), jnp.float32, -1.0, 1.0)
    base = 0.8 * jax.random.truncated_normal(level_keys[1], -4.0, 4.0, shape, jnp.float32)
    shared = 0.6 * jax.random.truncated_normal(level_keys[2], -3.0, 3.0, (1, TABLES, EMBED), jnp.float32)
    return ((base + shared) * jnp.exp(level)).astype(jnp.bfloat16)


def common_shift(key):
    keys = layout_keys(key)
    return jax.random.randint(keys[0], (N_LANE, N_GRP), 0, TABLES_DEV)


def common_lengths(key):
    keys = layout_keys(key)
    longest = jax.random.randint(keys[1], (DEVICES, 1, 1), 1, BAG_MAX + 1)
    raw_draw = jax.random.randint(keys[2], (DEVICES, BATCH_DEV, TABLES), 0, 1 << 20)
    lengths = (1 + raw_draw % longest).reshape(BATCH, TABLES)
    return lengths.at[0, 0].set(BAG_MAX).astype(jnp.int32)


def draw_bag_len(key, part):
    return common_lengths(key)


def draw_lookup_slot(key, part):
    keys = layout_keys(key)
    shift = common_shift(key)
    lengths = common_lengths(key)
    option_count = SLOTS // TABLES_DEV
    orders = jax.vmap(lambda one_key: jax.random.permutation(one_key, option_count))(jax.random.split(keys[3], N_LANE))
    shape = (BATCH, TABLES, BAG_MAX)
    first = jax.random.randint(keys[4], shape, 0, option_count)
    second = jax.random.randint(keys[5], shape, 0, option_count)
    third = jax.random.randint(keys[6], shape, 0, option_count)
    lowest = jnp.minimum(first, jnp.minimum(second, third))
    group_of = jnp.arange(BATCH, dtype=jnp.int32) // (BATCH_DEV * N_LANE)
    lane_of = jnp.arange(TABLES, dtype=jnp.int32) // TABLES_DEV
    table_local = jnp.arange(TABLES, dtype=jnp.int32) % TABLES_DEV
    picked = orders[lane_of[None, :, None], lowest]
    shift_here = shift[lane_of[None, :], group_of[:, None]]
    slot_number = picked * TABLES_DEV + ((table_local[None, :] - shift_here) % TABLES_DEV)[:, :, None]
    position = jnp.arange(BAG_MAX, dtype=jnp.int32)
    return jnp.where(position[None, None, :] < lengths[:, :, None], slot_number, -1).astype(jnp.int32)


def draw_slot_row(key, part):
    keys = layout_keys(key)
    shift = common_shift(key)
    slot_index = jnp.arange(SLOTS, dtype=jnp.int32).reshape(N_GRP, 1, 1, SLOTS_PEER)
    table_local = (slot_index + shift[None, :, :, None]) % TABLES_DEV
    shape = (N_GRP, N_LANE, N_GRP, SLOTS_PEER)
    hot_rows = jax.random.randint(keys[7], (N_GRP, N_LANE, 1, 8), 0, ROWS_DEV)
    sub_keys = jax.random.split(keys[8], 3)
    which = jax.random.randint(sub_keys[0], shape, 0, 8)
    hot_pick = jnp.take_along_axis(jnp.broadcast_to(hot_rows, (N_GRP, N_LANE, N_GRP, 8)), which, axis=3)
    drawn = jax.random.randint(sub_keys[1], shape, 0, ROWS_DEV)
    coin = jax.random.randint(sub_keys[2], shape, 0, 2)
    row_local = jnp.where(coin == 1, hot_pick, drawn)
    return (table_local * ROWS_DEV + row_local).astype(jnp.int32)


def block_levels(stream_key, shape, cuts, smallest, high):
    loudness, own = 1.0, jax.random.fold_in(stream_key, 6)
    for dim, parts in cuts:
        steps = jnp.exp(jax.random.uniform(jax.random.fold_in(own, dim), (parts,), jnp.float32, smallest / len(cuts), high / len(cuts)))
        loudness = loudness * jnp.repeat(steps, shape[dim] // parts).reshape([-1 if axis == dim else 1 for axis in range(len(shape))])
    return loudness


def noise(key, extent, width, bound, cuts=(), kind=jnp.bfloat16):
    values = jax.random.normal(key, extent, jnp.float32) * width
    if len(cuts) > 0:
        values = block_levels(key, extent, cuts, -0.22, 0.18) * values
    return jnp.clip(values, min=-bound, max=bound).astype(kind)


def setup_inputs(seed: int = 0) -> dict:
    seeds = jax.random.split(jax.random.key(seed), 7)
    grad_pooled = draw_grad_pooled(jax.random.fold_in(seeds[6], 71), 0)
    bag_len = draw_bag_len(jax.random.fold_in(seeds[6], 71), 0)
    lookup_slot = draw_lookup_slot(jax.random.fold_in(seeds[6], 71), 0)
    slot_row = draw_slot_row(jax.random.fold_in(seeds[6], 71), 0)
    weights = noise(seeds[4], (TABLES, ROWS, EMBED), 1.0, 6.0, ((0, 8), (1, 96)), jnp.float32)
    accum = jnp.clip(jnp.exp(math.log(0.5) - 2.3025851 * jax.random.uniform(seeds[5], (TABLES, ROWS), jnp.float32) ** block_levels(seeds[5], (TABLES, ROWS), ((0, 8), (1, 96)), -0.2, 0.2)), 0.05, 0.5)
    return {"grad_pooled": grad_pooled, "bag_len": bag_len, "lookup_slot": lookup_slot, "slot_row": slot_row, "weights": weights, "accum": accum}


def group_slot_sums(pieces):
    grad_block, length_block, slot_block = pieces
    scaled = (grad_block.astype(jnp.float32) / length_block.astype(jnp.float32)[:, :, None]).astype(jnp.bfloat16)
    values = scaled.astype(jnp.float32).reshape(N_LANE, BATCH_DEV, N_LANE, TABLES_DEV, 1, EMBED)
    slot_marks = slot_block.reshape(N_LANE, BATCH_DEV, N_LANE, TABLES_DEV, BAG_MAX)
    source_ids = jnp.arange(N_LANE, dtype=jnp.int32).reshape(N_LANE, 1, 1, 1, 1)
    target_ids = jnp.arange(N_LANE, dtype=jnp.int32).reshape(1, 1, N_LANE, 1, 1)
    dummy = N_LANE * N_LANE * SLOTS
    segment_ids = jnp.where(slot_marks >= 0, (source_ids * N_LANE + target_ids) * SLOTS + slot_marks, dummy)
    contrib = jnp.broadcast_to(values, (N_LANE, BATCH_DEV, N_LANE, TABLES_DEV, BAG_MAX, EMBED)).reshape(-1, EMBED)
    summed = jax.ops.segment_sum(contrib, segment_ids.reshape(-1).astype(jnp.int32), dummy + 1)
    partial_value = summed[:dummy].reshape(N_LANE, N_LANE, SLOTS, EMBED).astype(jnp.bfloat16)
    return lax.optimization_barrier(jnp.sum(partial_value.astype(jnp.float32), axis=0)).astype(jnp.bfloat16)

def reference(grad_pooled, bag_len, lookup_slot, slot_row, weights, accum):
    group_rows = N_LANE * BATCH_DEV
    slot_all = lax.map(group_slot_sums, (grad_pooled.reshape(N_GRP, group_rows, TABLES, EMBED), bag_len.reshape(N_GRP, group_rows, TABLES), lookup_slot.reshape(N_GRP, group_rows, TABLES, BAG_MAX)))
    local_index = jnp.transpose(slot_row, (2, 1, 0, 3))
    table_local = local_index // ROWS_DEV
    row_local = local_index % ROWS_DEV
    lane_ids = jnp.arange(N_LANE, dtype=jnp.int32).reshape(1, N_LANE, 1, 1)
    owner_ids = jnp.arange(N_GRP, dtype=jnp.int32).reshape(1, 1, N_GRP, 1)
    segment_ids = (lane_ids * TABLES_DEV + table_local) * ROWS + owner_ids * ROWS_DEV + row_local
    contrib = slot_all.astype(jnp.float32).reshape(-1, EMBED)
    row_grad = jax.ops.segment_sum(contrib, segment_ids.reshape(-1).astype(jnp.int32), TABLES * ROWS)
    row_grad = row_grad.reshape(TABLES, ROWS, EMBED)
    square_mean = lax.optimization_barrier(jnp.mean(row_grad * row_grad, axis=2))
    norm_total = EMBED * jnp.sum(square_mean)
    clip_limit = 0.5 * math.sqrt(DEVICES * SLOTS * EMBED)
    clip_factor = clip_limit / jnp.maximum(jnp.sqrt(norm_total), clip_limit)
    new_accum = accum + clip_factor * clip_factor * square_mean
    new_weights = weights - 0.3 * clip_factor * row_grad / (jnp.sqrt(new_accum)[:, :, None] + 1e-06)
    return (new_weights, new_accum)
```

```python
import math

import jax
import jax.numpy as jnp
from jax import lax
from jax.sharding import Mesh
from jax.sharding import PartitionSpec as P

SLOTS_PEER = 2
LANE = ("lane_0", "lane_1")
GRP = ("grp_0", "grp_1")
GRP_LANE = ("grp_0", "grp_1", "lane_0", "lane_1")


LEARN_RATE = 0.3
EPSILON = 1e-06


def gathered(x, axes):
    count = lax.axis_size(axes)
    copies = jnp.broadcast_to(x.reshape(1, 1, 128), (count, 1, 128))
    return lax.all_to_all(copies, axes, split_axis=0, concat_axis=0, tiled=True)


def sum_over_all(row):
    row = jnp.sum(gathered(row, ("grp_0", "lane_1")), axis=0)
    return jnp.sum(gathered(row, ("grp_1", "lane_0")))


def per_device(grad_pooled, bag_len, lookup_slot, slot_row, weights, accum):
    lane_count = lax.axis_size(LANE)
    group_count = lax.axis_size(GRP)
    number_slots = group_count * SLOTS_PEER
    batch_rows, table_count, embed_width = grad_pooled.shape
    tables_here = table_count // lane_count
    bag_depth = lookup_slot.shape[2]
    scaled = (grad_pooled.astype(jnp.float32) / bag_len.astype(jnp.float32)[:, :, None]).astype(
        jnp.bfloat16
    )
    arrived = lax.all_to_all(scaled, LANE, split_axis=1, concat_axis=0, tiled=True)
    values = arrived.reshape(lane_count, batch_rows * tables_here, embed_width)
    slot_marks = lookup_slot.reshape(lane_count, batch_rows * tables_here, bag_depth)
    numbers = lax.broadcasted_iota(jnp.int32, (1, number_slots, 1, 1), 1)
    counts = jnp.sum(slot_marks[:, None, :, :] == numbers, axis=-1, dtype=jnp.int32).astype(
        jnp.bfloat16
    )
    partial_value = jnp.einsum(
        "lsk,lke->lse", counts, values, preferred_element_type=jnp.float32
    ).astype(jnp.bfloat16)
    slot_sum = jnp.sum(partial_value.astype(jnp.float32), axis=0).astype(jnp.bfloat16)
    outgoing = slot_sum.reshape(group_count, SLOTS_PEER, embed_width)
    incoming = lax.all_to_all(outgoing, GRP, split_axis=0, concat_axis=0, tiled=True).reshape(
        number_slots, embed_width
    )
    targets = slot_row.reshape(1, number_slots)
    local_rows = accum.shape[0] * accum.shape[1]
    row_ids = lax.broadcasted_iota(jnp.int32, (local_rows, 1), 0)
    placing = (row_ids == targets).astype(jnp.bfloat16)
    row_grad = jnp.dot(placing, incoming, preferred_element_type=jnp.float32)
    square_mean = jnp.mean(row_grad * row_grad, axis=1)
    norm_row = jnp.sum(square_mean.reshape(-1, 128), axis=0)
    norm_total = embed_width * sum_over_all(norm_row)
    clip_limit = 0.5 * math.sqrt(group_count * lane_count * number_slots * embed_width)
    clip_factor = clip_limit / jnp.maximum(jnp.sqrt(norm_total), clip_limit)
    new_accum = accum + clip_factor * clip_factor * square_mean.reshape(accum.shape)
    step_rows = LEARN_RATE * clip_factor * row_grad.reshape(weights.shape)
    new_weights = weights - step_rows / (jnp.sqrt(new_accum)[:, :, None] + EPSILON)
    return (new_weights, new_accum)


def solution(mesh):
    torus = Mesh(mesh.devices.reshape(12, 8, 4, 2), ("grp_0", "grp_1", "lane_0", "lane_1"))
    in_specs = (
        P(GRP_LANE, None, None),
        P(GRP_LANE, None),
        P(GRP, LANE, None),
        P(GRP, LANE, None, None),
        P(LANE, GRP, None),
        P(LANE, GRP),
    )
    out_specs = (P(LANE, GRP, None), P(LANE, GRP))
    return jax.shard_map(
        per_device, mesh=torus, in_specs=in_specs, out_specs=out_specs, check_vma=False
    )
```

```python
import math

import jax
import jax.numpy as jnp
from jax import lax
from jax.experimental import pallas as pl
from jax.experimental.pallas import tpu as pltpu
from jax.sharding import Mesh
from jax.sharding import PartitionSpec as P


SLOTS_PEER = 2
LANE = ("lane_0", "lane_1")
GRP = ("grp_0", "grp_1")
GRP_LANE = ("grp_0", "grp_1", "lane_0", "lane_1")


LEARN_RATE = 0.3
EPSILON = 1e-06


def exchange(x, axes):
    return lax.all_to_all(x, axes, split_axis=0, concat_axis=0, tiled=True)


def gathered(x, axes):
    count = lax.axis_size(axes)
    return exchange(jnp.broadcast_to(x.reshape(1, 1, 128), (count, 1, 128)), axes)


def sum_over_all(row):
    row = jnp.sum(gathered(row, ("grp_0", "lane_1")), axis=0)
    return jnp.sum(gathered(row, ("grp_1", "lane_0")))


VMEM = pl.BlockSpec(memory_space=pltpu.VMEM)


def kernel_call(kernel, out_shape, flops, *args):
    moved = sum(x.size * x.dtype.itemsize for x in (*args, out_shape))
    return pl.pallas_call(
        kernel,
        out_shape=out_shape,
        in_specs=[VMEM] * len(args),
        out_specs=VMEM,
        compiler_params=pltpu.CompilerParams(vmem_limit_bytes=16 * 1024 * 1024),
        cost_estimate=pl.CostEstimate(flops=flops, bytes_accessed=moved, transcendentals=0),
    )(*args)


def marks_kernel(slot_ref, out_ref):
    chips, cores, tables, _, samples = out_ref.shape
    for chip in range(chips):
        for core in range(cores):
            start = (chip * cores + core) * samples
            for table in range(tables):
                out_ref[chip, core, table] = slot_ref[table, :, start : start + samples].astype(
                    out_ref.dtype
                )


def counts_kernel(marks_ref, out_ref):
    chips, cores, tables, depth, samples = marks_ref.shape
    slots = out_ref.shape[1]
    numbers = lax.broadcasted_iota(jnp.int32, (slots, samples), 0).astype(jnp.bfloat16)
    one, zero = jnp.bfloat16(1), jnp.bfloat16(0)
    for chip in range(chips):
        for core in range(cores):
            for table in range(tables):
                total = None
                for position in range(depth):
                    mark = marks_ref[chip, core, table, position : position + 1, :]
                    hit = jnp.where(numbers == mark, one, zero)
                    total = hit if total is None else total + hit
                start = (core * tables + table) * samples
                out_ref[chip, :, start : start + samples] = total


def sums_kernel(counts_ref, own_ref, pair_ref, out_ref):
    chips, _, terms = counts_ref.shape
    cores = lax.axis_size("lane_1")
    tables = own_ref.shape[0] // (chips * cores)
    width = own_ref.shape[2]
    core = lax.axis_index("lane_1")
    half = terms // cores
    for chip in range(chips):
        start = (chip * cores + core) * tables
        mine = pl.multiple_of(core * half, half)
        other = pl.multiple_of((1 - core) * half, half)
        out_ref[chip] = (
            jnp.dot(
                counts_ref[chip, :, pl.ds(mine, half)],
                own_ref[pl.ds(start, tables)].reshape(half, width),
                preferred_element_type=jnp.float32,
            )
            + jnp.dot(
                counts_ref[chip, :, pl.ds(other, half)],
                pair_ref[pl.ds(start, tables)].reshape(half, width),
                preferred_element_type=jnp.float32,
            )
        ).astype(out_ref.dtype)


def per_device(grad_pooled, bag_len, lookup_slot, slot_row, weights, accum):
    lane_count = lax.axis_size(LANE)
    chips, cores = lax.axis_size("lane_0"), lax.axis_size("lane_1")
    group_count = lax.axis_size(GRP)
    number_slots = group_count * SLOTS_PEER
    batch_rows, table_count, embed_width = grad_pooled.shape
    tables_here = table_count // lane_count
    bag_depth = lookup_slot.shape[2]
    marks = kernel_call(
        marks_kernel,
        jax.ShapeDtypeStruct((chips, cores, tables_here, bag_depth, batch_rows), jnp.bfloat16),
        lookup_slot.size,
        lookup_slot.transpose(1, 2, 0),
    )
    marks = exchange(marks, "lane_0")
    scaled = (
        grad_pooled.astype(jnp.float32) * (1.0 / bag_len.astype(jnp.float32))[:, :, None]
    ).astype(jnp.bfloat16)
    scaled = scaled.transpose(1, 0, 2)
    pair = lax.ppermute(scaled, "lane_1", [(0, 1), (1, 0)])
    terms = cores * tables_here * batch_rows
    counts = kernel_call(
        counts_kernel,
        jax.ShapeDtypeStruct((chips, number_slots, terms), jnp.bfloat16),
        chips * number_slots * terms * bag_depth,
        marks,
    )
    partial_value = kernel_call(
        sums_kernel,
        jax.ShapeDtypeStruct((chips, number_slots, embed_width), jnp.bfloat16),
        2 * chips * number_slots * terms * embed_width,
        counts,
        scaled,
        pair,
    )
    partial_value = exchange(partial_value, "lane_0")
    slot_sum = jnp.sum(partial_value.astype(jnp.float32), axis=0).astype(jnp.bfloat16)
    outgoing = slot_sum.reshape(group_count, SLOTS_PEER, embed_width)
    incoming = exchange(outgoing, GRP).reshape(number_slots, embed_width)
    targets = slot_row.reshape(1, number_slots)
    local_rows = accum.shape[0] * accum.shape[1]
    row_ids = lax.broadcasted_iota(jnp.int32, (local_rows, 1), 0)
    placing = (row_ids == targets).astype(jnp.bfloat16)
    row_grad = jnp.dot(placing, incoming, preferred_element_type=jnp.float32)
    square_mean = jnp.mean(row_grad * row_grad, axis=1)
    norm_row = jnp.sum(square_mean.reshape(-1, 128), axis=0)
    norm_total = embed_width * sum_over_all(norm_row)
    clip_limit = 0.5 * math.sqrt(group_count * lane_count * number_slots * embed_width)
    clip_factor = clip_limit / jnp.maximum(jnp.sqrt(norm_total), clip_limit)
    new_accum = accum + clip_factor * clip_factor * square_mean.reshape(accum.shape)
    step_rows = LEARN_RATE * clip_factor * row_grad.reshape(weights.shape)
    new_weights = weights - step_rows / (jnp.sqrt(new_accum)[:, :, None] + EPSILON)
    return (new_weights, new_accum)


def solution(mesh):
    torus = Mesh(mesh.devices.reshape(12, 8, 4, 2), ("grp_0", "grp_1", "lane_0", "lane_1"))
    in_specs = (
        P(GRP_LANE, None, None),
        P(GRP_LANE, None),
        P(GRP, LANE, None),
        P(GRP, LANE, None, None),
        P(LANE, GRP, None),
        P(LANE, GRP),
    )
    out_specs = (P(LANE, GRP, None), P(LANE, GRP))
    return jax.shard_map(
        per_device, mesh=torus, in_specs=in_specs, out_specs=out_specs, check_vma=False
    )
```

```python
import functools
import math

import jax
import jax.numpy as jnp
from jax import lax
from jax.experimental import pallas as pl
from jax.experimental.pallas import tpu as pltpu
from jax.sharding import Mesh
from jax.sharding import PartitionSpec as P


SLOTS_PEER = 2
LANE = ("lane_0", "lane_1")
GRP = ("grp_0", "grp_1")
GRP_LANE = ("grp_0", "grp_1", "lane_0", "lane_1")


LEARN_RATE = 0.3
EPSILON = 1e-06


def exchange(x, axes):
    return lax.all_to_all(x, axes, split_axis=0, concat_axis=0, tiled=True)


def gathered(x, axes):
    count = lax.axis_size(axes)
    return exchange(jnp.broadcast_to(x.reshape(1, 1, 128), (count, 1, 128)), axes)


def parts_of_sum(row):
    row = jnp.sum(gathered(row, ("grp_0", "lane_1")), axis=0)
    return gathered(row, ("grp_1", "lane_0"))


VMEM = pl.BlockSpec(memory_space=pltpu.VMEM)


def kernel_call(kernel, out_shape, flops, *args):
    moved = sum(x.size * x.dtype.itemsize for x in (*args, *jax.tree.leaves(out_shape)))
    return pl.pallas_call(
        kernel,
        out_shape=out_shape,
        in_specs=[VMEM] * len(args),
        out_specs=jax.tree.map(lambda _: VMEM, out_shape),
        compiler_params=pltpu.CompilerParams(vmem_limit_bytes=16 * 1024 * 1024),
        cost_estimate=pl.CostEstimate(flops=flops, bytes_accessed=moved, transcendentals=0),
    )(*args)


def marks_kernel(slot_ref, out_ref):
    chips, cores, tables, _, samples = out_ref.shape
    for chip in range(chips):
        for core in range(cores):
            start = (chip * cores + core) * samples
            for table in range(tables):
                out_ref[chip, core, table] = slot_ref[table, :, start : start + samples].astype(
                    out_ref.dtype
                )


def counts_kernel(marks_ref, out_ref):
    chips, cores, tables, depth, samples = marks_ref.shape
    slots = out_ref.shape[1]
    numbers = lax.broadcasted_iota(jnp.int32, (slots, samples), 0).astype(jnp.bfloat16)
    one, zero = jnp.bfloat16(1), jnp.bfloat16(0)
    for chip in range(chips):
        for core in range(cores):
            for table in range(tables):
                total = None
                for position in range(depth):
                    mark = marks_ref[chip, core, table, position : position + 1, :]
                    hit = jnp.where(numbers == mark, one, zero)
                    total = hit if total is None else total + hit
                start = (core * tables + table) * samples
                out_ref[chip, :, start : start + samples] = total


def other_half_kernel(scaled_ref, out_ref):
    chips, tables = out_ref.shape[:2]
    other = 1 - lax.axis_index("lane_1")
    for chip in range(chips):
        out_ref[chip] = scaled_ref[pl.ds((2 * chip + other) * tables, tables)]


def products(counts_ref, chip, core, values):
    tables, samples, width = values.shape
    start = pl.multiple_of(core * (tables * samples), tables * samples)
    return jnp.dot(
        counts_ref[chip, :, pl.ds(start, tables * samples)],
        values.reshape(tables * samples, width),
        preferred_element_type=jnp.float32,
    )


def own_kernel(counts_ref, scaled_ref, out_ref):
    core = lax.axis_index("lane_1")
    chips = counts_ref.shape[0]
    tables = scaled_ref.shape[0] // (2 * chips)
    for chip in range(chips):
        values = scaled_ref[pl.ds((2 * chip + core) * tables, tables)]
        out_ref[chip] = products(counts_ref, chip, core, values)


def pair_kernel(counts_ref, pair_ref, own_ref, out_ref):
    core = lax.axis_index("lane_1")
    for chip in range(counts_ref.shape[0]):
        both = own_ref[chip] + products(counts_ref, chip, 1 - core, pair_ref[chip])
        out_ref[chip] = both.astype(out_ref.dtype)


def update_kernel(scale, limit, norms_ref, square_ref, rows_ref, weights_ref, accum_ref, new_weights_ref, new_accum_ref):
    tables, _, _ = weights_ref.shape
    total = scale * jnp.sum(jnp.sum(norms_ref[...], axis=0), axis=(0, 1), keepdims=True)
    clip = limit / jnp.maximum(jnp.sqrt(total), limit)
    new_accum = accum_ref[...] + clip * clip * square_ref[...]
    new_accum_ref[...] = new_accum
    step = (LEARN_RATE * clip) / (jnp.sqrt(new_accum) + EPSILON)
    columns = jnp.transpose(jnp.concatenate([step, step], axis=0))
    for table in range(tables):
        new_weights_ref[table] = (
            weights_ref[table] - columns[:, table : table + 1] * rows_ref[table]
        )


def per_device(grad_pooled, bag_len, lookup_slot, slot_row, weights, accum):
    lane_count = lax.axis_size(LANE)
    chips, cores = lax.axis_size("lane_0"), lax.axis_size("lane_1")
    group_count = lax.axis_size(GRP)
    number_slots = group_count * SLOTS_PEER
    batch_rows, table_count, embed_width = grad_pooled.shape
    tables_here = table_count // lane_count
    bag_depth = lookup_slot.shape[2]
    marks = kernel_call(
        marks_kernel,
        jax.ShapeDtypeStruct((chips, cores, tables_here, bag_depth, batch_rows), jnp.bfloat16),
        lookup_slot.size,
        lookup_slot.transpose(1, 2, 0),
    )
    marks = exchange(marks, "lane_0")
    scaled = (grad_pooled.astype(jnp.float32) * (1.0 / bag_len.astype(jnp.float32))[:, :, None]).astype(jnp.bfloat16)
    scaled = scaled.transpose(1, 0, 2)
    half = jax.ShapeDtypeStruct((chips, tables_here, batch_rows, embed_width), jnp.bfloat16)
    pair = kernel_call(other_half_kernel, half, half.size, scaled)
    pair = lax.ppermute(pair, "lane_1", [(0, 1), (1, 0)])
    terms = cores * tables_here * batch_rows
    counts = kernel_call(
        counts_kernel,
        jax.ShapeDtypeStruct((chips, number_slots, terms), jnp.bfloat16),
        chips * number_slots * terms * bag_depth,
        marks,
    )
    flops = chips * number_slots * terms * embed_width
    part_shape = (chips, number_slots, embed_width)
    own = kernel_call(own_kernel, jax.ShapeDtypeStruct(part_shape, jnp.float32), flops, counts, scaled)
    own, targets = lax.optimization_barrier((own, slot_row.reshape(1, number_slots)))
    partial_value = kernel_call(pair_kernel, jax.ShapeDtypeStruct(part_shape, jnp.bfloat16), flops, counts, pair, own)
    partial_value = exchange(partial_value, "lane_0")
    slot_sum = jnp.sum(partial_value.astype(jnp.float32), axis=0).astype(jnp.bfloat16)
    outgoing = slot_sum.reshape(group_count, SLOTS_PEER, embed_width)
    incoming = exchange(outgoing, GRP).reshape(number_slots, embed_width)
    local_rows = accum.shape[0] * accum.shape[1]
    row_ids = lax.broadcasted_iota(jnp.int32, (local_rows, 1), 0)
    placing = (row_ids == targets).astype(jnp.bfloat16)
    row_grad = jnp.dot(placing, incoming, preferred_element_type=jnp.float32)
    square_mean = jnp.mean(row_grad * row_grad, axis=1)
    norm_row = jnp.sum(square_mean.reshape(-1, 128), axis=0)
    norm_row, square_mean = lax.optimization_barrier((norm_row, square_mean.reshape(accum.shape)))
    norms = parts_of_sum(norm_row)
    clip_limit = 0.5 * math.sqrt(group_count * lane_count * number_slots * embed_width)
    return kernel_call(
        functools.partial(update_kernel, embed_width, clip_limit),
        (
            jax.ShapeDtypeStruct(weights.shape, jnp.float32),
            jax.ShapeDtypeStruct(accum.shape, jnp.float32),
        ),
        2 * weights.size,
        norms,
        square_mean,
        row_grad.reshape(weights.shape),
        weights,
        accum,
    )


def solution(mesh):
    torus = Mesh(mesh.devices.reshape(12, 8, 4, 2), ("grp_0", "grp_1", "lane_0", "lane_1"))
    in_specs = (
        P(GRP_LANE, None, None),
        P(GRP_LANE, None),
        P(GRP, LANE, None),
        P(GRP, LANE, None, None),
        P(LANE, GRP, None),
        P(LANE, GRP),
    )
    out_specs = (P(LANE, GRP, None), P(LANE, GRP))
    return jax.shard_map(
        per_device, mesh=torus, in_specs=in_specs, out_specs=out_specs, check_vma=False
    )
```

```python
import functools
import math

import jax
import jax.numpy as jnp
from jax import lax
from jax.experimental import pallas as pl
from jax.experimental.pallas import tpu as pltpu
from jax.sharding import Mesh
from jax.sharding import PartitionSpec as P


SLOTS_PEER = 2
LANE = ("lane_0", "lane_1")
GRP = ("grp_0", "grp_1")
GRP_LANE = ("grp_0", "grp_1", "lane_0", "lane_1")


LEARN_RATE = 0.3
EPSILON = 1e-06


def exchange(x, axes):
    return lax.all_to_all(x, axes, split_axis=0, concat_axis=0, tiled=True)


def gathered(x, axes):
    count = lax.axis_size(axes)
    return exchange(jnp.broadcast_to(x.reshape(1, 1, 128), (count, 1, 128)), axes)


def parts_of_sum(row):
    row = jnp.sum(gathered(row, ("grp_0", "lane_1")), axis=0)
    return gathered(row, ("grp_1", "lane_0"))


VMEM = pl.BlockSpec(memory_space=pltpu.VMEM)


HBM = pl.BlockSpec(memory_space=pltpu.MemorySpace.HBM)


def kernel_call(kernel, out_shape, flops, *args, far_in=(), far_out=(), scratch=()):
    outs = jax.tree.leaves(out_shape)
    args = [
        pltpu.with_memory_space_constraint(x, pltpu.MemorySpace.HBM) if index in far_in else x
        for index, x in enumerate(args)
    ]
    moved = sum(x.size * x.dtype.itemsize for x in (*args, *outs))
    out_specs = [HBM if index in far_out else VMEM for index in range(len(outs))]
    return pl.pallas_call(
        kernel,
        out_shape=out_shape,
        in_specs=[HBM if index in far_in else VMEM for index in range(len(args))],
        out_specs=tuple(out_specs) if isinstance(out_shape, tuple) else out_specs[0],
        scratch_shapes=list(scratch),
        compiler_params=pltpu.CompilerParams(vmem_limit_bytes=16 * 1024 * 1024),
        cost_estimate=pl.CostEstimate(flops=flops, bytes_accessed=moved, transcendentals=0),
    )(*args)


def marks_kernel(far_slot_ref, far_length_ref, out_ref, share_ref, slot_ref, length_ref, arrived):
    lengths = pltpu.make_async_copy(far_length_ref, length_ref, arrived.at[0])
    slots = pltpu.make_async_copy(far_slot_ref, slot_ref, arrived.at[1])
    lengths.start()
    slots.start()
    lengths.wait()
    share_ref[...] = 1.0 / length_ref[...].astype(jnp.float32)
    slots.wait()
    chips, cores, tables, _, samples = out_ref.shape
    for chip in range(chips):
        for core in range(cores):
            start = (chip * cores + core) * samples
            for table in range(tables):
                out_ref[chip, core, table] = slot_ref[table, :, start : start + samples].astype(
                    out_ref.dtype
                )


def counts_kernel(marks_ref, out_ref):
    chips, cores, tables, depth, samples = marks_ref.shape
    slots = out_ref.shape[1]
    numbers = lax.broadcasted_iota(jnp.int32, (slots, samples), 0).astype(jnp.bfloat16)
    one, zero = jnp.bfloat16(1), jnp.bfloat16(0)
    for chip in range(chips):
        for core in range(cores):
            for table in range(tables):
                total = None
                for position in range(depth):
                    mark = marks_ref[chip, core, table, position : position + 1, :]
                    hit = jnp.where(numbers == mark, one, zero)
                    total = hit if total is None else total + hit
                start = (core * tables + table) * samples
                out_ref[chip, :, start : start + samples] = total


def other_half_kernel(scaled_ref, out_ref):
    chips, tables = out_ref.shape[:2]
    other = 1 - lax.axis_index("lane_1")
    for chip in range(chips):
        out_ref[chip] = scaled_ref[pl.ds((2 * chip + other) * tables, tables)]


def products(counts_ref, chip, core, values):
    tables, samples, width = values.shape
    start = pl.multiple_of(core * (tables * samples), tables * samples)
    return jnp.dot(
        counts_ref[chip, :, pl.ds(start, tables * samples)],
        values.reshape(tables * samples, width),
        preferred_element_type=jnp.float32,
    )


def own_kernel(counts_ref, scaled_ref, out_ref):
    core = lax.axis_index("lane_1")
    chips = counts_ref.shape[0]
    tables = scaled_ref.shape[0] // (2 * chips)
    for chip in range(chips):
        values = scaled_ref[pl.ds((2 * chip + core) * tables, tables)]
        out_ref[chip] = products(counts_ref, chip, core, values)


def pair_kernel(counts_ref, own_ref, pair_ref, out_ref, held, arrived):
    core = lax.axis_index("lane_1")
    chips = counts_ref.shape[0]
    copies = [
        pltpu.make_async_copy(pair_ref.at[chip], held.at[chip], arrived.at[chip]) for chip in range(chips)
    ]
    for copy in copies:
        copy.start()
    for chip in range(chips):
        copies[chip].wait()
        both = own_ref[chip] + products(counts_ref, chip, 1 - core, held[chip])
        out_ref[chip] = both.astype(out_ref.dtype)


def update_kernel(
    scale, limit, norms_ref, square_ref, rows_ref, weights_ref, accum_ref, new_weights_ref, new_accum_ref, done, sent
):
    tables = weights_ref.shape[0]
    total = scale * jnp.sum(jnp.sum(norms_ref[...], axis=0), axis=(0, 1), keepdims=True)
    clip = limit / jnp.maximum(jnp.sqrt(total), limit)
    new_accum = accum_ref[...] + clip * clip * square_ref[...]
    step = (LEARN_RATE * clip) / (jnp.sqrt(new_accum) + EPSILON)
    columns = jnp.transpose(jnp.concatenate([step, step], axis=0))
    copies = [
        pltpu.make_async_copy(done.at[table], new_weights_ref.at[table], sent.at[table])
        for table in range(tables)
    ]
    for table in range(tables):
        done[table] = weights_ref[table] - columns[:, table : table + 1] * rows_ref[table]
        copies[table].start()
    new_accum_ref[...] = new_accum
    for copy in copies:
        copy.wait()


def per_device(grad_pooled, bag_len, lookup_slot, slot_row, weights, accum):
    lane_count = lax.axis_size(LANE)
    chips, cores = lax.axis_size("lane_0"), lax.axis_size("lane_1")
    group_count = lax.axis_size(GRP)
    number_slots = group_count * SLOTS_PEER
    batch_rows, table_count, embed_width = grad_pooled.shape
    tables_here = table_count // lane_count
    bag_depth = lookup_slot.shape[2]
    marks, share = kernel_call(
        marks_kernel,
        (
            jax.ShapeDtypeStruct((chips, cores, tables_here, bag_depth, batch_rows), jnp.bfloat16),
            jax.ShapeDtypeStruct((table_count, batch_rows), jnp.float32),
        ),
        lookup_slot.size,
        lookup_slot.transpose(1, 2, 0),
        bag_len.transpose(1, 0),
        far_in=(0, 1),
        scratch=(
            pltpu.VMEM((tables_here, bag_depth, chips * cores * batch_rows), jnp.int32),
            pltpu.VMEM((table_count, batch_rows), jnp.int32),
            pltpu.SemaphoreType.DMA((2,)),
        ),
    )
    marks = exchange(marks, "lane_0")
    scaled = (grad_pooled.astype(jnp.float32) * share.transpose(1, 0)[:, :, None]).astype(jnp.bfloat16)
    scaled = scaled.transpose(1, 0, 2)
    half = jax.ShapeDtypeStruct((chips, tables_here, batch_rows, embed_width), jnp.bfloat16)
    pair = kernel_call(other_half_kernel, half, half.size, scaled)
    pair = lax.ppermute(pair, "lane_1", [(0, 1), (1, 0)])
    terms = cores * tables_here * batch_rows
    counts = kernel_call(
        counts_kernel,
        jax.ShapeDtypeStruct((chips, number_slots, terms), jnp.bfloat16),
        chips * number_slots * terms * bag_depth,
        marks,
    )
    flops = chips * number_slots * terms * embed_width
    part_shape = (chips, number_slots, embed_width)
    own = kernel_call(own_kernel, jax.ShapeDtypeStruct(part_shape, jnp.float32), flops, counts, scaled)
    own, targets = lax.optimization_barrier((own, slot_row.reshape(1, number_slots)))
    partial_value = kernel_call(
        pair_kernel,
        jax.ShapeDtypeStruct(part_shape, jnp.bfloat16),
        flops,
        counts,
        own,
        pair,
        far_in=(2,),
        scratch=(pltpu.VMEM(half.shape, half.dtype), pltpu.SemaphoreType.DMA((chips,))),
    )
    partial_value = exchange(partial_value, "lane_0")
    slot_sum = jnp.sum(partial_value.astype(jnp.float32), axis=0).astype(jnp.bfloat16)
    outgoing = slot_sum.reshape(group_count, SLOTS_PEER, embed_width)
    incoming = exchange(outgoing, GRP).reshape(number_slots, embed_width)
    local_rows = accum.shape[0] * accum.shape[1]
    row_ids = lax.broadcasted_iota(jnp.int32, (local_rows, 1), 0)
    placing = (row_ids == targets).astype(jnp.bfloat16)
    row_grad = jnp.dot(placing, incoming, preferred_element_type=jnp.float32)
    square_mean = jnp.mean(row_grad * row_grad, axis=1)
    norm_row = jnp.sum(square_mean.reshape(-1, 128), axis=0)
    norm_row, square_mean = lax.optimization_barrier((norm_row, square_mean.reshape(accum.shape)))
    norms = parts_of_sum(norm_row)
    clip_limit = 0.5 * math.sqrt(group_count * lane_count * number_slots * embed_width)
    return kernel_call(
        functools.partial(update_kernel, embed_width, clip_limit),
        (
            jax.ShapeDtypeStruct(weights.shape, jnp.float32),
            jax.ShapeDtypeStruct(accum.shape, jnp.float32),
        ),
        2 * weights.size,
        norms,
        square_mean,
        row_grad.reshape(weights.shape),
        weights,
        accum,
        far_out=(0,),
        scratch=(pltpu.VMEM(weights.shape, weights.dtype), pltpu.SemaphoreType.DMA((tables_here,))),
    )


def solution(mesh):
    torus = Mesh(mesh.devices.reshape(12, 8, 4, 2), ("grp_0", "grp_1", "lane_0", "lane_1"))
    in_specs = (
        P(GRP_LANE, None, None),
        P(GRP_LANE, None),
        P(GRP, LANE, None),
        P(GRP, LANE, None, None),
        P(LANE, GRP, None),
        P(LANE, GRP),
    )
    out_specs = (P(LANE, GRP, None), P(LANE, GRP))
    return jax.shard_map(
        per_device, mesh=torus, in_specs=in_specs, out_specs=out_specs, check_vma=False
    )
```

```python
import functools
import math

import jax
import jax.numpy as jnp
from jax import lax
from jax.experimental import pallas as pl
from jax.experimental.pallas import tpu as pltpu
from jax.sharding import Mesh
from jax.sharding import PartitionSpec as P


SLOTS_PEER = 2
LANE = ("lane_0", "lane_1")
GRP = ("grp_0", "grp_1")
GRP_LANE = ("grp_0", "grp_1", "lane_0", "lane_1")


LEARN_RATE = 0.3
EPSILON = 1e-06


def exchange(x, axes):
    return lax.all_to_all(x, axes, split_axis=0, concat_axis=0, tiled=True)


def gathered(x, axes):
    count = lax.axis_size(axes)
    return exchange(jnp.broadcast_to(x.reshape(1, 1, 128), (count, 1, 128)), axes)


def parts_of_sum(row):
    row = jnp.sum(gathered(row, ("grp_0", "lane_1")), axis=0)
    return gathered(row, ("grp_1", "lane_0"))


VMEM = pl.BlockSpec(memory_space=pltpu.VMEM)


HBM = pl.BlockSpec(memory_space=pltpu.MemorySpace.HBM)


def kernel_call(kernel, out_shape, flops, *args, far_in=(), scratch=()):
    outs = jax.tree.leaves(out_shape)
    args = [
        pltpu.with_memory_space_constraint(x, pltpu.MemorySpace.HBM) if index in far_in else x
        for index, x in enumerate(args)
    ]
    moved = sum(x.size * x.dtype.itemsize for x in (*args, *outs))
    return pl.pallas_call(
        kernel,
        out_shape=out_shape,
        in_specs=[HBM if index in far_in else VMEM for index in range(len(args))],
        out_specs=jax.tree.map(lambda _: VMEM, out_shape),
        scratch_shapes=list(scratch),
        compiler_params=pltpu.CompilerParams(vmem_limit_bytes=16 * 1024 * 1024),
        cost_estimate=pl.CostEstimate(flops=flops, bytes_accessed=moved, transcendentals=0),
    )(*args)


def marks_kernel(far_slot_ref, far_length_ref, out_ref, share_ref, slot_ref, length_ref, arrived):
    lengths = pltpu.make_async_copy(far_length_ref, length_ref, arrived.at[0])
    slots = pltpu.make_async_copy(far_slot_ref, slot_ref, arrived.at[1])
    lengths.start()
    slots.start()
    lengths.wait()
    share_ref[...] = 1.0 / length_ref[...].astype(jnp.float32)
    slots.wait()
    chips, cores, tables, _, samples = out_ref.shape
    for chip in range(chips):
        for core in range(cores):
            start = (chip * cores + core) * samples
            for table in range(tables):
                out_ref[chip, core, table] = slot_ref[table, :, start : start + samples].astype(
                    out_ref.dtype
                )


def counts_kernel(marks_ref, out_ref):
    chips, cores, tables, depth, samples = marks_ref.shape
    slots = out_ref.shape[1]
    numbers = lax.broadcasted_iota(jnp.int32, (slots, samples), 0).astype(jnp.bfloat16)
    one, zero = jnp.bfloat16(1), jnp.bfloat16(0)
    for chip in range(chips):
        for core in range(cores):
            for table in range(tables):
                total = None
                for position in range(depth):
                    mark = marks_ref[chip, core, table, position : position + 1, :]
                    hit = jnp.where(numbers == mark, one, zero)
                    total = hit if total is None else total + hit
                start = (core * tables + table) * samples
                out_ref[chip, :, start : start + samples] = total


def halves_kernel(scaled_ref, own_ref, other_ref):
    chips, tables = own_ref.shape[:2]
    core = lax.axis_index("lane_1")
    for chip in range(chips):
        own_ref[chip] = scaled_ref[pl.ds((2 * chip + core) * tables, tables)]
        other_ref[chip] = scaled_ref[pl.ds((2 * chip + 1 - core) * tables, tables)]


def products(counts_ref, chip, core, values):
    tables, samples, width = values.shape
    start = pl.multiple_of(core * (tables * samples), tables * samples)
    return jnp.dot(
        counts_ref[chip, :, pl.ds(start, tables * samples)],
        values.reshape(tables * samples, width),
        preferred_element_type=jnp.float32,
    )


def own_kernel(counts_ref, values_ref, out_ref):
    core = lax.axis_index("lane_1")
    for chip in range(counts_ref.shape[0]):
        out_ref[chip] = products(counts_ref, chip, core, values_ref[chip])


def pair_kernel(counts_ref, pair_ref, own_ref, out_ref):
    core = lax.axis_index("lane_1")
    for chip in range(counts_ref.shape[0]):
        both = own_ref[chip] + products(counts_ref, chip, 1 - core, pair_ref[chip])
        out_ref[chip] = both.astype(out_ref.dtype)


def update_kernel(scale, limit, norms_ref, square_ref, rows_ref, weights_ref, accum_ref, new_weights_ref, new_accum_ref):
    tables, _, _ = weights_ref.shape
    total = scale * jnp.sum(jnp.sum(norms_ref[...], axis=0), axis=(0, 1), keepdims=True)
    clip = limit / jnp.maximum(jnp.sqrt(total), limit)
    new_accum = accum_ref[...] + clip * clip * square_ref[...]
    new_accum_ref[...] = new_accum
    step = (LEARN_RATE * clip) / (jnp.sqrt(new_accum) + EPSILON)
    columns = jnp.transpose(jnp.concatenate([step, step], axis=0))
    for table in range(tables):
        new_weights_ref[table] = (
            weights_ref[table] - columns[:, table : table + 1] * rows_ref[table]
        )


def per_device(grad_pooled, bag_len, lookup_slot, slot_row, weights, accum):
    lane_count = lax.axis_size(LANE)
    chips, cores = lax.axis_size("lane_0"), lax.axis_size("lane_1")
    group_count = lax.axis_size(GRP)
    number_slots = group_count * SLOTS_PEER
    batch_rows, table_count, embed_width = grad_pooled.shape
    tables_here = table_count // lane_count
    bag_depth = lookup_slot.shape[2]
    marks, share = kernel_call(
        marks_kernel,
        (
            jax.ShapeDtypeStruct((chips, cores, tables_here, bag_depth, batch_rows), jnp.bfloat16),
            jax.ShapeDtypeStruct((table_count, batch_rows), jnp.float32),
        ),
        lookup_slot.size,
        lookup_slot.transpose(1, 2, 0),
        bag_len.transpose(1, 0),
        far_in=(0, 1),
        scratch=(
            pltpu.VMEM((tables_here, bag_depth, chips * cores * batch_rows), jnp.int32),
            pltpu.VMEM((table_count, batch_rows), jnp.int32),
            pltpu.SemaphoreType.DMA((2,)),
        ),
    )
    marks = exchange(marks, "lane_0")
    scaled = (grad_pooled.astype(jnp.float32) * share.transpose(1, 0)[:, :, None]).astype(jnp.bfloat16)
    scaled = scaled.transpose(1, 0, 2)
    half = jax.ShapeDtypeStruct((chips, tables_here, batch_rows, embed_width), jnp.bfloat16)
    values, other = kernel_call(halves_kernel, (half, half), 2 * half.size, scaled)
    pair = lax.ppermute(other, "lane_1", [(0, 1), (1, 0)])
    terms = cores * tables_here * batch_rows
    counts = kernel_call(
        counts_kernel,
        jax.ShapeDtypeStruct((chips, number_slots, terms), jnp.bfloat16),
        chips * number_slots * terms * bag_depth,
        marks,
    )
    flops = chips * number_slots * terms * embed_width
    part_shape = (chips, number_slots, embed_width)
    own = kernel_call(own_kernel, jax.ShapeDtypeStruct(part_shape, jnp.float32), flops, counts, values)
    own, targets = lax.optimization_barrier((own, slot_row.reshape(1, number_slots)))
    partial_value = kernel_call(pair_kernel, jax.ShapeDtypeStruct(part_shape, jnp.bfloat16), flops, counts, pair, own)
    partial_value = exchange(partial_value, "lane_0")
    slot_sum = jnp.sum(partial_value.astype(jnp.float32), axis=0).astype(jnp.bfloat16)
    outgoing = slot_sum.reshape(group_count, SLOTS_PEER, embed_width)
    incoming = exchange(outgoing, GRP).reshape(number_slots, embed_width)
    local_rows = accum.shape[0] * accum.shape[1]
    row_ids = lax.broadcasted_iota(jnp.int32, (local_rows, 1), 0)
    placing = (row_ids == targets).astype(jnp.bfloat16)
    row_grad = jnp.dot(placing, incoming, preferred_element_type=jnp.float32)
    square_mean = jnp.mean(row_grad * row_grad, axis=1)
    norm_row = jnp.sum(square_mean.reshape(-1, 128), axis=0)
    norm_row, square_mean = lax.optimization_barrier((norm_row, square_mean.reshape(accum.shape)))
    norms = parts_of_sum(norm_row)
    clip_limit = 0.5 * math.sqrt(group_count * lane_count * number_slots * embed_width)
    return kernel_call(
        functools.partial(update_kernel, embed_width, clip_limit),
        (
            jax.ShapeDtypeStruct(weights.shape, jnp.float32),
            jax.ShapeDtypeStruct(accum.shape, jnp.float32),
        ),
        2 * weights.size,
        norms,
        square_mean,
        row_grad.reshape(weights.shape),
        weights,
        accum,
    )


def solution(mesh):
    torus = Mesh(mesh.devices.reshape(12, 8, 4, 2), ("grp_0", "grp_1", "lane_0", "lane_1"))
    in_specs = (
        P(GRP_LANE, None, None),
        P(GRP_LANE, None),
        P(GRP, LANE, None),
        P(GRP, LANE, None, None),
        P(LANE, GRP, None),
        P(LANE, GRP),
    )
    out_specs = (P(LANE, GRP, None), P(LANE, GRP))
    return jax.shard_map(
        per_device, mesh=torus, in_specs=in_specs, out_specs=out_specs, check_vma=False
    )
```

```python
import functools
import math

import jax
import jax.numpy as jnp
import numpy as np
from jax import lax
from jax.experimental import pallas as pl
from jax.experimental.pallas import tpu as pltpu
from jax.sharding import Mesh
from jax.sharding import PartitionSpec as P


SLOTS_PEER = 2
LANE = ("lane_0", "lane_1")
GRP = ("grp_0", "grp_1")
GRP_LANE = ("grp_0", "grp_1", "lane_0", "lane_1")


FAR, FAR_Y = 10, 9

LEARN_RATE = 0.3
EPSILON = 1e-06


def exchange(x, axes):
    return lax.all_to_all(x, axes, split_axis=0, concat_axis=0, tiled=True)


def exchange_from(x, axes, begin):
    count = lax.axis_size(axes)
    first = count * begin // 16
    order = np.roll(np.arange(count), -first).tolist()
    x = jnp.concatenate([x[first:], x[:first]], axis=0)
    x = lax.all_to_all(x, axes, split_axis=0, concat_axis=0, tiled=True, axis_index_groups=[order])
    return jnp.concatenate([x[count - first :], x[: count - first]], axis=0)


def gathered(x, axes, begin):
    sizes = [lax.axis_size(axis) for axis in GRP_LANE]
    count = lax.axis_size(axes)
    places = np.arange(math.prod(sizes)).reshape(sizes)
    inner = [index for index, axis in enumerate(GRP_LANE) if axis in axes]
    outer = [index for index, axis in enumerate(GRP_LANE) if axis not in axes]
    groups = np.roll(places.transpose(outer + inner).reshape(-1, count), -(count * begin // 16), axis=1).tolist()
    copies = jnp.broadcast_to(x.reshape(1, 1, 128), (count, 1, 128))
    return lax.all_to_all(copies, GRP_LANE, split_axis=0, concat_axis=0, tiled=True, axis_index_groups=groups)


def parts_of_sum(row):
    row = jnp.sum(gathered(row, ("grp_0", "lane_1"), FAR), axis=0)
    return gathered(row, ("grp_1", "lane_0"), FAR_Y)


VMEM = pl.BlockSpec(memory_space=pltpu.VMEM)


HBM = pl.BlockSpec(memory_space=pltpu.MemorySpace.HBM)


def kernel_call(kernel, out_shape, flops, *args, far_in=(), scratch=()):
    outs = jax.tree.leaves(out_shape)
    args = [
        pltpu.with_memory_space_constraint(x, pltpu.MemorySpace.HBM) if index in far_in else x
        for index, x in enumerate(args)
    ]
    moved = sum(x.size * x.dtype.itemsize for x in (*args, *outs))
    return pl.pallas_call(
        kernel,
        out_shape=out_shape,
        in_specs=[HBM if index in far_in else VMEM for index in range(len(args))],
        out_specs=jax.tree.map(lambda _: VMEM, out_shape),
        scratch_shapes=list(scratch),
        compiler_params=pltpu.CompilerParams(vmem_limit_bytes=16 * 1024 * 1024),
        cost_estimate=pl.CostEstimate(flops=flops, bytes_accessed=moved, transcendentals=0),
    )(*args)


def marks_kernel(far_slot_ref, far_length_ref, out_ref, share_ref, slot_ref, length_ref, arrived):
    lengths = pltpu.make_async_copy(far_length_ref, length_ref, arrived.at[0])
    slots = pltpu.make_async_copy(far_slot_ref, slot_ref, arrived.at[1])
    lengths.start()
    slots.start()
    lengths.wait()
    share_ref[...] = 1.0 / length_ref[...].astype(jnp.float32)
    slots.wait()
    chips, cores, tables, _, samples = out_ref.shape
    for chip in range(chips):
        for core in range(cores):
            start = (chip * cores + core) * samples
            for table in range(tables):
                out_ref[chip, core, table] = slot_ref[table, :, start : start + samples].astype(
                    out_ref.dtype
                )


def counts_kernel(marks_ref, out_ref):
    chips, cores, tables, depth, samples = marks_ref.shape
    slots = out_ref.shape[1]
    numbers = lax.broadcasted_iota(jnp.int32, (slots, samples), 0).astype(jnp.bfloat16)
    one, zero = jnp.bfloat16(1), jnp.bfloat16(0)
    for chip in range(chips):
        for core in range(cores):
            for table in range(tables):
                total = None
                for position in range(depth):
                    mark = marks_ref[chip, core, table, position : position + 1, :]
                    hit = jnp.where(numbers == mark, one, zero)
                    total = hit if total is None else total + hit
                start = (core * tables + table) * samples
                out_ref[chip, :, start : start + samples] = total


def halves_kernel(scaled_ref, own_ref, other_ref):
    chips, tables = own_ref.shape[:2]
    core = lax.axis_index("lane_1")
    for chip in range(chips):
        own_ref[chip] = scaled_ref[pl.ds((2 * chip + core) * tables, tables)]
        other_ref[chip] = scaled_ref[pl.ds((2 * chip + 1 - core) * tables, tables)]


def products(counts_ref, chip, core, values):
    tables, samples, width = values.shape
    start = pl.multiple_of(core * (tables * samples), tables * samples)
    return jnp.dot(
        counts_ref[chip, :, pl.ds(start, tables * samples)],
        values.reshape(tables * samples, width),
        preferred_element_type=jnp.float32,
    )


def own_kernel(counts_ref, values_ref, out_ref):
    core = lax.axis_index("lane_1")
    for chip in range(counts_ref.shape[0]):
        out_ref[chip] = products(counts_ref, chip, core, values_ref[chip])


def pair_kernel(counts_ref, pair_ref, own_ref, out_ref):
    core = lax.axis_index("lane_1")
    for chip in range(counts_ref.shape[0]):
        both = own_ref[chip] + products(counts_ref, chip, 1 - core, pair_ref[chip])
        out_ref[chip] = both.astype(out_ref.dtype)


def update_kernel(scale, limit, norms_ref, square_ref, rows_ref, weights_ref, accum_ref, new_weights_ref, new_accum_ref):
    tables, _, _ = weights_ref.shape
    total = scale * jnp.sum(jnp.sum(norms_ref[...], axis=0), axis=(0, 1), keepdims=True)
    clip = limit / jnp.maximum(jnp.sqrt(total), limit)
    new_accum = accum_ref[...] + clip * clip * square_ref[...]
    new_accum_ref[...] = new_accum
    step = (LEARN_RATE * clip) / (jnp.sqrt(new_accum) + EPSILON)
    columns = jnp.transpose(jnp.concatenate([step, step], axis=0))
    for table in range(tables):
        new_weights_ref[table] = (
            weights_ref[table] - columns[:, table : table + 1] * rows_ref[table]
        )


def per_device(grad_pooled, bag_len, lookup_slot, slot_row, weights, accum):
    lane_count = lax.axis_size(LANE)
    chips, cores = lax.axis_size("lane_0"), lax.axis_size("lane_1")
    group_count = lax.axis_size(GRP)
    number_slots = group_count * SLOTS_PEER
    batch_rows, table_count, embed_width = grad_pooled.shape
    tables_here = table_count // lane_count
    bag_depth = lookup_slot.shape[2]
    marks, share = kernel_call(
        marks_kernel,
        (
            jax.ShapeDtypeStruct((chips, cores, tables_here, bag_depth, batch_rows), jnp.bfloat16),
            jax.ShapeDtypeStruct((table_count, batch_rows), jnp.float32),
        ),
        lookup_slot.size,
        lookup_slot.transpose(1, 2, 0),
        bag_len.transpose(1, 0),
        far_in=(0, 1),
        scratch=(
            pltpu.VMEM((tables_here, bag_depth, chips * cores * batch_rows), jnp.int32),
            pltpu.VMEM((table_count, batch_rows), jnp.int32),
            pltpu.SemaphoreType.DMA((2,)),
        ),
    )
    marks = exchange(marks, "lane_0")
    scaled = (grad_pooled.astype(jnp.float32) * share.transpose(1, 0)[:, :, None]).astype(jnp.bfloat16)
    scaled = scaled.transpose(1, 0, 2)
    half = jax.ShapeDtypeStruct((chips, tables_here, batch_rows, embed_width), jnp.bfloat16)
    values, other = kernel_call(halves_kernel, (half, half), 2 * half.size, scaled)
    pair = lax.ppermute(other, "lane_1", [(0, 1), (1, 0)])
    terms = cores * tables_here * batch_rows
    counts = kernel_call(
        counts_kernel,
        jax.ShapeDtypeStruct((chips, number_slots, terms), jnp.bfloat16),
        chips * number_slots * terms * bag_depth,
        marks,
    )
    flops = chips * number_slots * terms * embed_width
    part_shape = (chips, number_slots, embed_width)
    own = kernel_call(own_kernel, jax.ShapeDtypeStruct(part_shape, jnp.float32), flops, counts, values)
    own, targets = lax.optimization_barrier((own, slot_row.reshape(1, number_slots)))
    partial_value = kernel_call(pair_kernel, jax.ShapeDtypeStruct(part_shape, jnp.bfloat16), flops, counts, pair, own)
    partial_value = exchange(partial_value, "lane_0")
    slot_sum = jnp.sum(partial_value.astype(jnp.float32), axis=0).astype(jnp.bfloat16)
    outgoing = slot_sum.reshape(group_count, SLOTS_PEER, embed_width)
    incoming = exchange_from(outgoing, GRP, FAR).reshape(number_slots, embed_width)
    local_rows = accum.shape[0] * accum.shape[1]
    row_ids = lax.broadcasted_iota(jnp.int32, (local_rows, 1), 0)
    placing = (row_ids == targets).astype(jnp.bfloat16)
    row_grad = jnp.dot(placing, incoming, preferred_element_type=jnp.float32)
    square_mean = jnp.mean(row_grad * row_grad, axis=1)
    norm_row = jnp.sum(square_mean.reshape(-1, 128), axis=0)
    norm_row, square_mean = lax.optimization_barrier((norm_row, square_mean.reshape(accum.shape)))
    norms = parts_of_sum(norm_row)
    clip_limit = 0.5 * math.sqrt(group_count * lane_count * number_slots * embed_width)
    return kernel_call(
        functools.partial(update_kernel, embed_width, clip_limit),
        (
            jax.ShapeDtypeStruct(weights.shape, jnp.float32),
            jax.ShapeDtypeStruct(accum.shape, jnp.float32),
        ),
        2 * weights.size,
        norms,
        square_mean,
        row_grad.reshape(weights.shape),
        weights,
        accum,
    )


def solution(mesh):
    torus = Mesh(mesh.devices.reshape(12, 8, 4, 2), ("grp_0", "grp_1", "lane_0", "lane_1"))
    in_specs = (
        P(GRP_LANE, None, None),
        P(GRP_LANE, None),
        P(GRP, LANE, None),
        P(GRP, LANE, None, None),
        P(LANE, GRP, None),
        P(LANE, GRP),
    )
    out_specs = (P(LANE, GRP, None), P(LANE, GRP))
    return jax.shard_map(
        per_device, mesh=torus, in_specs=in_specs, out_specs=out_specs, check_vma=False
    )
```

```python
import functools
import math

import jax
import jax.numpy as jnp
import numpy as np
from jax import lax
from jax.experimental import pallas as pl
from jax.experimental.pallas import tpu as pltpu
from jax.sharding import Mesh
from jax.sharding import PartitionSpec as P


SLOTS_PEER = 2
LANE = ("lane_0", "lane_1")
GRP = ("grp_0", "grp_1")
GRP_LANE = ("grp_0", "grp_1", "lane_0", "lane_1")


FAR, FAR_Y, FAR_X = 10, 9, 2

LEARN_RATE = 0.3
EPSILON = 1e-06


def exchange_along_x(x):
    chips = lax.axis_size("lane_0")
    order = [(FAR_X + place) % chips for place in range(chips)]
    return lax.all_to_all(x, "lane_0", split_axis=0, concat_axis=0, tiled=True, axis_index_groups=[order])


def exchange_from(x, axes, begin):
    count = lax.axis_size(axes)
    first = count * begin // 16
    order = np.roll(np.arange(count), -first).tolist()
    x = jnp.concatenate([x[first:], x[:first]], axis=0)
    x = lax.all_to_all(x, axes, split_axis=0, concat_axis=0, tiled=True, axis_index_groups=[order])
    return jnp.concatenate([x[count - first :], x[: count - first]], axis=0)


def gathered(x, axes, begin):
    sizes = [lax.axis_size(axis) for axis in GRP_LANE]
    count = lax.axis_size(axes)
    places = np.arange(math.prod(sizes)).reshape(sizes)
    inner = [index for index, axis in enumerate(GRP_LANE) if axis in axes]
    outer = [index for index, axis in enumerate(GRP_LANE) if axis not in axes]
    groups = np.roll(places.transpose(outer + inner).reshape(-1, count), -(count * begin // 16), axis=1).tolist()
    copies = jnp.broadcast_to(x.reshape(1, 1, 128), (count, 1, 128))
    return lax.all_to_all(copies, GRP_LANE, split_axis=0, concat_axis=0, tiled=True, axis_index_groups=groups)


def parts_of_sum(row):
    row = jnp.sum(gathered(row, ("grp_0", "lane_1"), FAR), axis=0)
    return gathered(row, ("grp_1", "lane_0"), FAR_Y)


VMEM = pl.BlockSpec(memory_space=pltpu.VMEM)


HBM = pl.BlockSpec(memory_space=pltpu.MemorySpace.HBM)


def kernel_call(kernel, out_shape, flops, *args, far_in=(), scratch=()):
    outs = jax.tree.leaves(out_shape)
    args = [
        pltpu.with_memory_space_constraint(x, pltpu.MemorySpace.HBM) if index in far_in else x
        for index, x in enumerate(args)
    ]
    moved = sum(x.size * x.dtype.itemsize for x in (*args, *outs))
    return pl.pallas_call(
        kernel,
        out_shape=out_shape,
        in_specs=[HBM if index in far_in else VMEM for index in range(len(args))],
        out_specs=jax.tree.map(lambda _: VMEM, out_shape),
        scratch_shapes=list(scratch),
        compiler_params=pltpu.CompilerParams(vmem_limit_bytes=16 * 1024 * 1024),
        cost_estimate=pl.CostEstimate(flops=flops, bytes_accessed=moved, transcendentals=0),
    )(*args)


def marks_kernel(far_slot_ref, far_length_ref, out_ref, share_ref, slot_ref, length_ref, arrived):
    lengths = pltpu.make_async_copy(far_length_ref, length_ref, arrived.at[0])
    slots = pltpu.make_async_copy(far_slot_ref, slot_ref, arrived.at[1])
    lengths.start()
    slots.start()
    lengths.wait()
    share_ref[...] = 1.0 / length_ref[...].astype(jnp.float32)
    slots.wait()
    chips, cores, tables, _, samples = out_ref.shape
    for chip in range(chips):
        for core in range(cores):
            start = (chip * cores + core) * samples
            for table in range(tables):
                out_ref[(chip - FAR_X) % chips, core, table] = slot_ref[table, :, start : start + samples].astype(
                    out_ref.dtype
                )


def counts_kernel(marks_ref, out_ref):
    chips, cores, tables, depth, samples = marks_ref.shape
    slots = out_ref.shape[1]
    numbers = lax.broadcasted_iota(jnp.int32, (slots, samples), 0).astype(jnp.bfloat16)
    one, zero = jnp.bfloat16(1), jnp.bfloat16(0)
    for chip in range(chips):
        for core in range(cores):
            for table in range(tables):
                total = None
                for position in range(depth):
                    mark = marks_ref[(chip - FAR_X) % chips, core, table, position : position + 1, :]
                    hit = jnp.where(numbers == mark, one, zero)
                    total = hit if total is None else total + hit
                start = (core * tables + table) * samples
                out_ref[chip, :, start : start + samples] = total


def halves_kernel(scaled_ref, own_ref, other_ref):
    chips, tables = own_ref.shape[:2]
    core = lax.axis_index("lane_1")
    for chip in range(chips):
        own_ref[chip] = scaled_ref[pl.ds((2 * chip + core) * tables, tables)]
        other_ref[chip] = scaled_ref[pl.ds((2 * chip + 1 - core) * tables, tables)]


def products(counts_ref, chip, core, values):
    tables, samples, width = values.shape
    start = pl.multiple_of(core * (tables * samples), tables * samples)
    return jnp.dot(
        counts_ref[chip, :, pl.ds(start, tables * samples)],
        values.reshape(tables * samples, width),
        preferred_element_type=jnp.float32,
    )


def own_kernel(counts_ref, values_ref, out_ref):
    core = lax.axis_index("lane_1")
    for chip in range(counts_ref.shape[0]):
        out_ref[chip] = products(counts_ref, chip, core, values_ref[chip])


def pair_kernel(counts_ref, pair_ref, own_ref, out_ref):
    core = lax.axis_index("lane_1")
    chips = counts_ref.shape[0]
    for chip in range(chips):
        both = own_ref[chip] + products(counts_ref, chip, 1 - core, pair_ref[chip])
        out_ref[(chip - FAR_X) % chips] = both.astype(out_ref.dtype)


def update_kernel(scale, limit, norms_ref, square_ref, rows_ref, weights_ref, accum_ref, new_weights_ref, new_accum_ref):
    tables, _, _ = weights_ref.shape
    total = scale * jnp.sum(jnp.sum(norms_ref[...], axis=0), axis=(0, 1), keepdims=True)
    clip = limit / jnp.maximum(jnp.sqrt(total), limit)
    new_accum = accum_ref[...] + clip * clip * square_ref[...]
    new_accum_ref[...] = new_accum
    step = (LEARN_RATE * clip) / (jnp.sqrt(new_accum) + EPSILON)
    columns = jnp.transpose(jnp.concatenate([step, step], axis=0))
    for table in range(tables):
        new_weights_ref[table] = (
            weights_ref[table] - columns[:, table : table + 1] * rows_ref[table]
        )


def per_device(grad_pooled, bag_len, lookup_slot, slot_row, weights, accum):
    lane_count = lax.axis_size(LANE)
    chips, cores = lax.axis_size("lane_0"), lax.axis_size("lane_1")
    group_count = lax.axis_size(GRP)
    number_slots = group_count * SLOTS_PEER
    batch_rows, table_count, embed_width = grad_pooled.shape
    tables_here = table_count // lane_count
    bag_depth = lookup_slot.shape[2]
    marks, share = kernel_call(
        marks_kernel,
        (
            jax.ShapeDtypeStruct((chips, cores, tables_here, bag_depth, batch_rows), jnp.bfloat16),
            jax.ShapeDtypeStruct((table_count, batch_rows), jnp.float32),
        ),
        lookup_slot.size,
        lookup_slot.transpose(1, 2, 0),
        bag_len.transpose(1, 0),
        far_in=(0, 1),
        scratch=(
            pltpu.VMEM((tables_here, bag_depth, chips * cores * batch_rows), jnp.int32),
            pltpu.VMEM((table_count, batch_rows), jnp.int32),
            pltpu.SemaphoreType.DMA((2,)),
        ),
    )
    marks = exchange_along_x(marks)
    scaled = (grad_pooled.astype(jnp.float32) * share.transpose(1, 0)[:, :, None]).astype(jnp.bfloat16)
    scaled = scaled.transpose(1, 0, 2)
    half = jax.ShapeDtypeStruct((chips, tables_here, batch_rows, embed_width), jnp.bfloat16)
    values, other = kernel_call(halves_kernel, (half, half), 2 * half.size, scaled)
    pair = lax.ppermute(other, "lane_1", [(0, 1), (1, 0)])
    terms = cores * tables_here * batch_rows
    counts = kernel_call(
        counts_kernel,
        jax.ShapeDtypeStruct((chips, number_slots, terms), jnp.bfloat16),
        chips * number_slots * terms * bag_depth,
        marks,
    )
    flops = chips * number_slots * terms * embed_width
    part_shape = (chips, number_slots, embed_width)
    own = kernel_call(own_kernel, jax.ShapeDtypeStruct(part_shape, jnp.float32), flops, counts, values)
    own, targets = lax.optimization_barrier((own, slot_row.reshape(1, number_slots)))
    partial_value = kernel_call(pair_kernel, jax.ShapeDtypeStruct(part_shape, jnp.bfloat16), flops, counts, pair, own)
    partial_value = exchange_along_x(partial_value)
    slot_sum = jnp.sum(partial_value.astype(jnp.float32), axis=0).astype(jnp.bfloat16)
    outgoing = slot_sum.reshape(group_count, SLOTS_PEER, embed_width)
    incoming = exchange_from(outgoing, GRP, FAR).reshape(number_slots, embed_width)
    local_rows = accum.shape[0] * accum.shape[1]
    row_ids = lax.broadcasted_iota(jnp.int32, (local_rows, 1), 0)
    placing = (row_ids == targets).astype(jnp.bfloat16)
    row_grad = jnp.dot(placing, incoming, preferred_element_type=jnp.float32)
    square_mean = jnp.mean(row_grad * row_grad, axis=1)
    norm_row = jnp.sum(square_mean.reshape(-1, 128), axis=0)
    norm_row, square_mean = lax.optimization_barrier((norm_row, square_mean.reshape(accum.shape)))
    norms = parts_of_sum(norm_row)
    clip_limit = 0.5 * math.sqrt(group_count * lane_count * number_slots * embed_width)
    return kernel_call(
        functools.partial(update_kernel, embed_width, clip_limit),
        (
            jax.ShapeDtypeStruct(weights.shape, jnp.float32),
            jax.ShapeDtypeStruct(accum.shape, jnp.float32),
        ),
        2 * weights.size,
        norms,
        square_mean,
        row_grad.reshape(weights.shape),
        weights,
        accum,
    )


def solution(mesh):
    torus = Mesh(mesh.devices.reshape(12, 8, 4, 2), ("grp_0", "grp_1", "lane_0", "lane_1"))
    in_specs = (
        P(GRP_LANE, None, None),
        P(GRP_LANE, None),
        P(GRP, LANE, None),
        P(GRP, LANE, None, None),
        P(LANE, GRP, None),
        P(LANE, GRP),
    )
    out_specs = (P(LANE, GRP, None), P(LANE, GRP))
    return jax.shard_map(
        per_device, mesh=torus, in_specs=in_specs, out_specs=out_specs, check_vma=False
    )
```
